256 devices in a mesh: seq: 32 (over x, y, core), head: 8 (over z).
Axes of the slice: x: 4, y: 4, z: 8, core: 2. Of those that a mesh axis runs over, the one named last changes fastest.
Arguments:
- query_rows: bfloat16 [32768, 4096], P(('seq', 'head')), may hold values from -1.796875 to 1.796875
- key_rows: bfloat16 [32768, 4096], P(('seq', 'head')), may hold values from -1.796875 to 1.796875
- value_rows: bfloat16 [32768, 4096], P(('seq', 'head')), may hold values from -1.796875 to 1.796875
- out_grad: bfloat16 [32768, 4096], P(('seq', 'head')), may hold values from -1.796875 to 1.796875
- decay: float32 [32, 32768], P('head', 'seq'), may hold values from 0 to 2
Outputs:
- attended: bfloat16 [32768, 4096], P(('seq', 'head'))
- query_grad: bfloat16 [32768, 4096], P(('seq', 'head'))
- key_grad: bfloat16 [32768, 4096], P(('seq', 'head'))
- value_grad: bfloat16 [32768, 4096], P(('seq', 'head'))
The draws below stay inside these ranges and needn't reach their ends.
All inputs are finite; a program needn't handle non-finite values.
Results may differ from the reference program's by a relative error of at most 0.0083.
Values may be sent and summed in bfloat16 or wider, within the bound.
A program may use at most 128 MiB of HBM per device.

```python
import jax
import jax.numpy as jnp
from jax import lax

E = 128
BLOCK = 1024
HEAD_COUNT = 32
SEQUENCE_TOKENS = 32768
N_SEQ = 32


def draw_decay(key, part):
    random_subkeys = jax.random.split(key, 8)
    quick_share = 0.25
    middle_share = 0.25
    slow_low = 0.3
    head_draw = jax.random.uniform(random_subkeys[0], (HEAD_COUNT,))
    quick_heads = head_draw < quick_share
    middle_heads = jnp.logical_and(head_draw >= quick_share, head_draw < quick_share + middle_share)
    quick_rate = jnp.exp(jax.random.uniform(random_subkeys[1], (HEAD_COUNT,), minval=jnp.log(0.015), maxval=jnp.log(0.04)))
    middle_rate = jnp.exp(jax.random.uniform(random_subkeys[7], (HEAD_COUNT,), minval=jnp.log(0.15), maxval=0.0)) / BLOCK
    slow_rate = jnp.exp(jax.random.uniform(random_subkeys[2], (HEAD_COUNT,), minval=jnp.log(slow_low), maxval=jnp.log(0.9))) / SEQUENCE_TOKENS
    baseline_rate = jnp.where(quick_heads, quick_rate, jnp.where(middle_heads, middle_rate, slow_rate))
    blocks = SEQUENCE_TOKENS // BLOCK
    block_multiplier = jnp.exp(jax.random.uniform(random_subkeys[3], (HEAD_COUNT, blocks), minval=jnp.log(0.5), maxval=jnp.log(2.0)))
    block_multiplier = jnp.repeat(block_multiplier, BLOCK, axis=1)
    token_multiplier = jax.random.uniform(random_subkeys[4], (HEAD_COUNT, SEQUENCE_TOKENS), minval=0.5, maxval=1.5)
    spike_locations = jax.random.randint(random_subkeys[5], (HEAD_COUNT, 2), 0, SEQUENCE_TOKENS)
    spike_loss = jax.random.uniform(random_subkeys[6], (HEAD_COUNT, 2), minval=0.22, maxval=0.69)
    token_positions = jnp.arange(SEQUENCE_TOKENS)
    spike_events = jnp.sum(jnp.where(token_positions[None, None, :] == spike_locations[:, :, None], spike_loss[:, :, None], 0.0), axis=1)
    return (baseline_rate[:, None] * block_multiplier * token_multiplier + spike_events).astype(jnp.float32)


def block_scale(key, shape, shards, low, top_value):
    def one(axis_at, blocks):
        steps = jax.random.uniform(jax.random.fold_in(jax.random.fold_in(key, 6), axis_at), (blocks,), jnp.float32, low / len(shards), top_value / len(shards))
        return jnp.repeat(jnp.exp(steps), shape[axis_at] // blocks).reshape((-1,) + (1,) * (len(shape) - axis_at - 1))

    loudness = one(*shards[0])
    for cut in shards[1:]:
        loudness = loudness * one(*cut)
    return loudness


def gaussian(stream_key, dims, spread, limit, pieces=(), held_as=jnp.bfloat16):
    entries = jax.random.normal(stream_key, dims, jnp.float32) * spread
    if len(pieces) > 0:
        entries = block_scale(stream_key, dims, pieces, -0.22, 0.18) * entries
    return jnp.clip(entries, min=-limit, max=limit).astype(held_as)


def setup_inputs(seed: int = 0) -> dict:
    key_list = jax.random.split(jax.random.key(seed), 6)
    query_rows = gaussian(key_list[0], (SEQUENCE_TOKENS, HEAD_COUNT * E), 0.3, 1.796875, ((0, 256),))
    key_rows = gaussian(key_list[1], (SEQUENCE_TOKENS, HEAD_COUNT * E), 0.3, 1.796875, ((0, 256),))
    value_rows = gaussian(key_list[2], (SEQUENCE_TOKENS, HEAD_COUNT * E), 0.3, 1.796875, ((0, 256),))
    out_grad = gaussian(key_list[3], (SEQUENCE_TOKENS, HEAD_COUNT * E), 0.3, 1.796875, ((0, 256),))
    decay = draw_decay(jax.random.fold_in(key_list[5], 71), 0)
    return {"query_rows": query_rows, "key_rows": key_rows, "value_rows": value_rows, "out_grad": out_grad, "decay": decay}


def rounded(values):
    return lax.optimization_barrier(values.astype(jnp.bfloat16)).astype(jnp.float32)


def rows_by_block(array):
    return array.reshape(N_SEQ, BLOCK, HEAD_COUNT, E).transpose(0, 2, 1, 3)


def block_summary(items):
    query_part, key_part, value_part, grad_part, decay_rates = items
    scale_factor = E ** -0.5
    running = jnp.cumsum(decay_rates, axis=1)
    block_log = running[:, -1]
    weights = jnp.exp(-(block_log[:, None] - running))
    growth = jnp.exp(-running)
    keyed = rounded(key_part.astype(jnp.float32) * weights[:, :, None])
    queried = rounded(query_part.astype(jnp.float32) * growth[:, :, None])
    update = jnp.einsum('hcd,hce->hde', keyed, value_part.astype(jnp.float32))
    source = scale_factor * jnp.einsum('hcd,hce->hde', queried, grad_part.astype(jnp.float32))
    return block_log, update, source


def block_result(items):
    query_part, key_part, value_part, grad_part, decay_rates, state_in, state_grad = items
    scale_factor = E ** -0.5
    running = jnp.cumsum(decay_rates, axis=1)
    block_log = running[:, -1]
    weights = jnp.exp(-(block_log[:, None] - running))
    growth = jnp.exp(-running)
    length = decay_rates.shape[1]
    causal = (jnp.arange(length)[:, None] >= jnp.arange(length)[None, :])[None]
    spread_log = running[:, :, None] - running[:, None, :]
    decay_mask = jnp.where(causal, jnp.exp(-jnp.where(causal, spread_log, 0.0)), 0.0)
    query_f = query_part.astype(jnp.float32)
    key_f = key_part.astype(jnp.float32)
    value_f = value_part.astype(jnp.float32)
    grad_f = grad_part.astype(jnp.float32)
    state_half = rounded(state_in)
    grad_half = rounded(state_grad)
    scores = rounded(scale_factor * jnp.einsum('htd,hsd->hts', query_f, key_f) * decay_mask)
    grad_scores = rounded(scale_factor * jnp.einsum('hte,hse->hts', grad_f, value_f) * decay_mask)
    attended = jnp.einsum('hts,hse->hte', scores, value_f) + scale_factor * growth[:, :, None] * jnp.einsum('htd,hde->hte', query_f, state_half)
    query_grad = jnp.einsum('hts,hsd->htd', grad_scores, key_f) + scale_factor * growth[:, :, None] * jnp.einsum('hte,hde->htd', grad_f, state_half)
    key_grad = jnp.einsum('hts,htd->hsd', grad_scores, query_f) + weights[:, :, None] * jnp.einsum('hse,hde->hsd', value_f, grad_half)
    value_grad = jnp.einsum('hts,hte->hse', scores, grad_f) + weights[:, :, None] * jnp.einsum('hsd,hde->hse', key_f, grad_half)
    return (attended.astype(jnp.bfloat16), query_grad.astype(jnp.bfloat16), key_grad.astype(jnp.bfloat16), value_grad.astype(jnp.bfloat16))


def forward_step(state, items):
    block_log, update = items
    return jnp.exp(-block_log)[:, None, None] * state + update, state


def backward_step(state, items):
    block_log, source = items
    return source + jnp.exp(-block_log)[:, None, None] * state, state


def reference(query_rows, key_rows, value_rows, out_grad, decay):
    query_blocks = rows_by_block(query_rows)
    key_blocks = rows_by_block(key_rows)
    value_blocks = rows_by_block(value_rows)
    grad_blocks = rows_by_block(out_grad)
    decay_blocks = decay.reshape(HEAD_COUNT, N_SEQ, BLOCK).transpose(1, 0, 2)
    block_logs, updates, sources = lax.map(block_summary, (query_blocks, key_blocks, value_blocks, grad_blocks, decay_blocks))
    zero_state = jnp.zeros((HEAD_COUNT, E, E), jnp.float32)
    _, states_in = lax.scan(forward_step, zero_state, (block_logs, updates))
    _, states_grad = lax.scan(backward_step, zero_state, (block_logs, sources), reverse=True)
    results = lax.map(block_result, (query_blocks, key_blocks, value_blocks, grad_blocks, decay_blocks, states_in, states_grad))
    merged = tuple(part.transpose(0, 2, 1, 3).reshape(SEQUENCE_TOKENS, HEAD_COUNT * E) for part in results)
    return (merged[0], merged[1], merged[2], merged[3])
```

```python
import functools

import jax
import jax.numpy as jnp
from jax import lax
from jax.experimental import pallas as pl
from jax.experimental.pallas import tpu as pltpu
from jax.sharding import PartitionSpec as P

E = 128
SCALE = E ** -0.5
GH = 4
HC = 2
LAG = 2
ROWS = 8
MESH = pl.DeviceIdType.MESH
F32 = jnp.float32
BF16 = jnp.bfloat16


def total_wait(ref, count, sem):
    part = ref.at[pl.ds(0, count)]
    pltpu.make_async_copy(part, part, sem).wait()


def barrier_with(peers):
    barrier = pltpu.get_barrier_semaphore()
    for peer in peers:
        pl.semaphore_signal(barrier, inc=1, device_id=peer, device_id_type=MESH)
    pl.semaphore_wait(barrier, len(peers))


def decay_kernel(nz, nrow, nx, decay_ref, dz_ref, lb_ref, lx_ref, msg, dz, bl, lb, rs, lx,
                 s_dz, r_dz, s_lb, r_lb, s_lx, r_lx):
    z = lax.axis_index("head")
    sq = lax.axis_index("seq")
    x = sq // nrow
    m = sq % nrow
    z_peers = [(z + i) % nz for i in range(1, nz)]
    m_peers = [(m + i) % nrow for i in range(1, nrow)]
    x_peers = [(x + i) % nx for i in range(1, nx)]
    barrier_with([(sq, p) for p in z_peers] + [(x * nrow + p, z) for p in m_peers]
                 + [(p * nrow + m, z) for p in x_peers])
    run = decay_ref[...]
    length = run.shape[1]
    lane = lax.broadcasted_iota(jnp.int32, run.shape, 1)
    shift = 1
    while shift < length:
        run = run + jnp.where(lane >= shift, pltpu.roll(run, shift, 1), 0.0)
        shift *= 2
    block_log = jnp.broadcast_to(run[:, length - 1:], (GH, E))
    start = jnp.zeros((GH, E), F32)
    for p in range(nz):
        part = run[:, p * E:(p + 1) * E]
        end = jnp.broadcast_to(part[:, E - 1:], (GH, E))
        msg[p, 0:GH, :] = part
        msg[p, GH:2 * GH, :] = start
        msg[p, 2 * GH:3 * GH, :] = block_log
        msg[p, 3 * GH:, :] = end
        start = end
    bl[0:GH, :] = block_log
    bl[GH:, :] = jnp.zeros((8 - GH, E), F32)
    copies = []
    for i, p in enumerate(m_peers):
        copies.append(pltpu.make_async_remote_copy(
            bl, lb.at[m], s_lb.at[i], r_lb, device_id=(x * nrow + p, z), device_id_type=MESH))
        copies[-1].start()
    for i, p in enumerate(z_peers):
        copies.append(pltpu.make_async_remote_copy(
            msg.at[p], dz.at[z], s_dz.at[i], r_dz, device_id=(sq, p), device_id_type=MESH))
        copies[-1].start()
    dz[pl.ds(z, 1)] = msg[pl.ds(z, 1)]
    lb[pl.ds(m, 1)] = bl[...][None]
    total_wait(lb, nrow - 1, r_lb)
    rs[...] = jnp.sum(lb[...], axis=0)
    for i, p in enumerate(x_peers):
        copies.append(pltpu.make_async_remote_copy(
            rs, lx.at[x], s_lx.at[i], r_lx, device_id=(p * nrow + m, z), device_id_type=MESH))
        copies[-1].start()
    lx[pl.ds(x, 1)] = rs[...][None]
    total_wait(dz, nz - 1, r_dz)
    total_wait(lx, nx - 1, r_lx)
    dz_ref[...] = dz[...]
    lb_ref[...] = lb[...]
    lx_ref[...] = lx[...]
    for copy in copies:
        copy.wait_send()


def run_decay(decay, nz, nrow, nx):
    vm = pl.BlockSpec(memory_space=pltpu.VMEM)
    dma = pltpu.SemaphoreType.DMA
    return pl.pallas_call(
        functools.partial(decay_kernel, nz, nrow, nx),
        out_shape=(jax.ShapeDtypeStruct((nz, 4 * GH, E), F32),
                   jax.ShapeDtypeStruct((nrow, 8, E), F32),
                   jax.ShapeDtypeStruct((nx, 8, E), F32)),
        in_specs=[vm],
        out_specs=(vm, vm, vm),
        scratch_shapes=[
            pltpu.VMEM((nz, 4 * GH, E), F32), pltpu.VMEM((nz, 4 * GH, E), F32),
            pltpu.VMEM((8, E), F32), pltpu.VMEM((nrow, 8, E), F32),
            pltpu.VMEM((8, E), F32), pltpu.VMEM((nx, 8, E), F32),
            dma((nz - 1,)), dma, dma((nrow - 1,)), dma, dma((nx - 1,)), dma,
        ],
        compiler_params=pltpu.CompilerParams(collective_id=1, has_side_effects=True),
        name="decay_exchange",
    )(decay)


def column_of(row):
    return jnp.transpose(jnp.broadcast_to(row, (E, E)))


def tdot(a, b):
    return lax.dot_general(a, b, (((0,), (0,)), ((), ())), preferred_element_type=F32)


def ntdot(a, b):
    return lax.dot_general(a, b, (((1,), (1,)), ((), ())), preferred_element_type=F32)


def dot(a, b):
    return jnp.dot(a, b, preferred_element_type=F32)


def update_kernel(heads, q_ref, k_ref, v_ref, g_ref, r_ref, c_ref, u_ref):
    for i in range(heads):
        cols = pl.ds(i * E, E)
        r_col = column_of(r_ref[i])
        keyed = (k_ref[:, cols].astype(F32) * jnp.exp(r_col - c_ref[i])).astype(BF16)
        queried = (q_ref[:, cols].astype(F32) * jnp.exp(-r_col)).astype(BF16)
        u_ref[0, i] = tdot(keyed, v_ref[:, cols]).astype(BF16)
        u_ref[1, i] = (SCALE * tdot(queried, g_ref[:, cols])).astype(BF16)


def run_update(q, k, v, g, r, c, heads=4):
    n = r.shape[0]
    tok = pl.BlockSpec((E, heads * E), lambda i: (0, i))
    row = pl.BlockSpec((heads, 1, E), lambda i: (i, 0, 0))
    return pl.pallas_call(
        functools.partial(update_kernel, heads),
        grid=(n // heads,),
        out_shape=jax.ShapeDtypeStruct((2, n, E, E), BF16),
        in_specs=[tok, tok, tok, tok, row, row],
        out_specs=pl.BlockSpec((2, heads, E, E), lambda i: (0, i, 0, 0)),
        name="chunk_updates",
    )(q, k, v, g, r[:, None], c[:, None])


def output_kernel(heads, q_ref, k_ref, v_ref, g_ref, r_ref, c_ref, s_ref,
                  a_ref, dq_ref, dk_ref, dv_ref):
    t_at = lax.broadcasted_iota(jnp.int32, (E, E), 0)
    s_at = lax.broadcasted_iota(jnp.int32, (E, E), 1)
    causal = t_at >= s_at
    for i in range(heads):
        cols = pl.ds(i * E, E)
        q, k, v, g = q_ref[:, cols], k_ref[:, cols], v_ref[:, cols], g_ref[:, cols]
        r_row = r_ref[i]
        r_col = column_of(r_row)
        mask = jnp.where(causal, jnp.exp(jnp.where(causal, r_row - r_col, 0.0)), 0.0) * SCALE
        growth = SCALE * jnp.exp(-r_col)
        weight = jnp.exp(r_col - c_ref[i])
        scores = (ntdot(q, k) * mask).astype(BF16)
        grads = (ntdot(g, v) * mask).astype(BF16)
        state, back = s_ref[0, i], s_ref[1, i]
        a_ref[:, cols] = (dot(scores, v) + growth * dot(q, state)).astype(BF16)
        dq_ref[:, cols] = (dot(grads, k) + growth * ntdot(g, state)).astype(BF16)
        dk_ref[:, cols] = (tdot(grads, q) + weight * ntdot(v, back)).astype(BF16)
        dv_ref[:, cols] = (tdot(scores, g) + weight * dot(k, back)).astype(BF16)


def run_output(q, k, v, g, r, c, states, heads=4):
    n = r.shape[0]
    tok = pl.BlockSpec((E, heads * E), lambda i: (0, i))
    row = pl.BlockSpec((heads, 1, E), lambda i: (i, 0, 0))
    return pl.pallas_call(
        functools.partial(output_kernel, heads),
        grid=(n // heads,),
        out_shape=(jax.ShapeDtypeStruct(q.shape, BF16),) * 4,
        in_specs=[tok, tok, tok, tok, row, row,
                  pl.BlockSpec((2, heads, E, E), lambda i: (0, i, 0, 0))],
        out_specs=(tok, tok, tok, tok),
        name="chunk_outputs",
    )(q, k, v, g, r[:, None], c[:, None], states)


def state_kernel(nz, nrow, nx, plan, u_ref, chain_ref, suf_ref, pre_ref, eb_ref, ex_ref, out_ref,
                 rs_in, rs_out, tot, ta, rxo, rx, so, sa, ch_in, ch_out,
                 rs_s, rs_r, ta_s, ta_r, rx_s, rx_r, so_s, so_r, ag_s, ag_r, ch_s, ch_r):
    z = lax.axis_index("head")
    sq = lax.axis_index("seq")
    x = sq // nrow
    m = sq % nrow
    right = (z + 1) % nz
    left = (z + nz - 1) % nz
    heads = nz * GH
    chunks = heads // HC
    cut = E // nrow
    toward = ((sq, right), (sq, left))
    m_peers = [(m + i) % nrow for i in range(1, nrow)]
    x_peers = [(x + i) % nx for i in range(1, nx)]
    barrier_with(list(toward) + [(x * nrow + p, z) for p in m_peers] + [(p * nrow + m, z) for p in x_peers])

    before = (suf_ref, pre_ref)
    after = (pre_ref, suf_ref)
    pending = []

    def hops(way, t):
        return nz // 2 if way == t else nz // 2 - 1

    def sign(way):
        return 1 if way == 0 else -1

    for t in range(2):
        place = z if t == 0 else nz - 1 - z

        @pl.when(place == 0)
        def _(t=t):
            def clear(h, _):
                ch_in[t, h] = jnp.zeros((E, E), BF16)
                return 0
            lax.fori_loop(0, heads, clear, 0)

    def chain_copy(t, c):
        part = pl.ds(c * HC, HC)
        return pltpu.make_async_remote_copy(
            ch_out.at[t, part], ch_in.at[t, part], ch_s.at[t, c], ch_r.at[t, c],
            device_id=toward[t], device_id_type=MESH)

    def chain_step(step, _):
        for t in range(2):
            place = z if t == 0 else nz - 1 - z
            c = step - LAG * place

            @pl.when((c >= 0) & (c < chunks))
            def _(t=t, place=place, c=c):
                @pl.when(place > 0)
                def _():
                    chain_copy(t, c).wait_recv()

                @pl.when(place < nz - 1)
                def _():
                    for i in range(HC):
                        h = c * HC + i
                        nxt = chain_ref[h] * ch_in[t, h].astype(F32) + u_ref[t, h].astype(F32)
                        ch_out[t, h] = nxt.astype(BF16)
                    chain_copy(t, c).start()
        return 0

    chain_at = [0]

    def chain_run(count):
        if count > 0:
            lax.fori_loop(chain_at[0], chain_at[0] + count, chain_step, 0)
            chain_at[0] += count

    for s in range(nz // 2):
        for t in range(2):
            for way in range(2):
                k = hops(way, t)
                if s >= k:
                    continue
                group = (z + sign(way) * (k - s) + nz) % nz
                if s > 0:
                    pltpu.make_async_remote_copy(
                        rs_out.at[way, t, s - 1], rs_in.at[way, t, s - 1], rs_s.at[way, t, s - 1],
                        rs_r.at[way, t, s - 1], device_id=toward[way], device_id_type=MESH).wait_recv()

                def fill(i, _, way=way, t=t, s=s, group=group):
                    h = group * GH + i
                    val = before[t][h] * u_ref[t, h].astype(F32)
                    if s > 0:
                        val = val + rs_in[way, t, s - 1, i].astype(F32)
                    rs_out[way, t, s, i] = val.astype(BF16)
                    return 0
                lax.fori_loop(0, GH, fill, 0)
                copy = pltpu.make_async_remote_copy(
                    rs_out.at[way, t, s], rs_in.at[way, t, s], rs_s.at[way, t, s], rs_r.at[way, t, s],
                    device_id=toward[way], device_id_type=MESH)
                copy.start()
                pending.append(copy)
        chain_run(plan[0][s])
    for t in range(2):
        for way in range(2):
            k = hops(way, t)
            pltpu.make_async_remote_copy(
                rs_out.at[way, t, k - 1], rs_in.at[way, t, k - 1], rs_s.at[way, t, k - 1],
                rs_r.at[way, t, k - 1], device_id=toward[way], device_id_type=MESH).wait_recv()

        def finish(i, _, t=t):
            h = z * GH + i
            val = before[t][h] * u_ref[t, h].astype(F32)
            for way in range(2):
                val = val + rs_in[way, t, hops(way, t) - 1, i].astype(F32)
            tot[t, i] = val.astype(BF16)
            return 0
        lax.fori_loop(0, GH, finish, 0)

    for i, p in enumerate(m_peers):
        copy = pltpu.make_async_remote_copy(
            tot.at[:, :, pl.ds(p * cut, cut), :], ta.at[m], ta_s.at[i], ta_r,
            device_id=(x * nrow + p, z), device_id_type=MESH)
        copy.start()
        pending.append(copy)
    ta[pl.ds(m, 1)] = tot[:, :, pl.ds(pl.multiple_of(m * cut, cut), cut), :][None]
    chain_run(plan[1][0])
    total_wait(ta, nrow - 1, ta_r)
    order = (list(range(nrow)), list(range(nrow))[::-1])
    for t in range(2):
        for i in range(GH):
            acc = ta[order[t][0], t, i].astype(F32)
            for b in order[t][1:]:
                acc = eb_ref[b, i:i + 1, :] * acc + ta[b, t, i].astype(F32)
            rxo[t, i] = acc.astype(BF16)
    for i, p in enumerate(x_peers):
        copy = pltpu.make_async_remote_copy(
            rxo, rx.at[x], rx_s.at[i], rx_r, device_id=(p * nrow + m, z), device_id_type=MESH)
        copy.start()
        pending.append(copy)
    chain_run(plan[1][1])
    total_wait(rx, nx - 1, rx_r)
    for t in range(2):
        for i in range(GH):
            acc = jnp.zeros((cut, E), F32)
            for b in (range(nx) if t == 0 else range(nx - 1, -1, -1)):
                use = (b < x) if t == 0 else (b > x)
                new = ex_ref[b, i:i + 1, :] * acc + rx[b, t, i].astype(F32)
                acc = jnp.where(use, new, acc)
            for b in order[t]:
                so[b, t, i] = acc.astype(BF16)
                acc = eb_ref[b, i:i + 1, :] * acc + ta[b, t, i].astype(F32)
    rows = pl.ds(pl.multiple_of(m * cut, cut), cut)
    for i, p in enumerate(m_peers):
        copy = pltpu.make_async_remote_copy(
            so.at[p], sa.at[z, :, :, rows, :], so_s.at[i], so_r,
            device_id=(x * nrow + p, z), device_id_type=MESH)
        copy.start()
        pending.append(copy)
    sa[pl.ds(z, 1), :, :, rows, :] = so[pl.ds(m, 1)]
    chain_run(plan[1][2])
    total_wait(so, nrow - 1, so_r)

    for s in range(nz // 2):
        for t in range(2):
            for way in range(2):
                k = hops(way, t)
                if s >= k:
                    continue
                group = (z - sign(way) * s + nz) % nz

                def ag_copy(group, at, way=way, t=t):
                    return pltpu.make_async_remote_copy(
                        sa.at[group, t], sa.at[group, t], ag_s.at[way, t, at], ag_r.at[way, t, at],
                        device_id=toward[way], device_id_type=MESH)
                if s > 0:
                    ag_copy(group, s - 1).wait_recv()
                copy = ag_copy(group, s)
                copy.start()
                pending.append(copy)
        chain_run(plan[2][s])
    chain_run(chunks + LAG * (nz - 1) - chain_at[0])
    for t in range(2):
        for way in range(2):
            k = hops(way, t)
            group = (z - sign(way) * k + nz) % nz
            pltpu.make_async_remote_copy(
                sa.at[group, t], sa.at[group, t], ag_s.at[way, t, k - 1], ag_r.at[way, t, k - 1],
                device_id=toward[way], device_id_type=MESH).wait_recv()

        def combine(h, _, t=t):
            val = after[t][h] * sa[h // GH, t, h % GH].astype(F32) + ch_in[t, h].astype(F32)
            out_ref[t, h] = val.astype(BF16)
            return 0
        lax.fori_loop(0, heads, combine, 0)

    for copy in pending:
        copy.wait_send()

    def drain(c, _):
        for t in range(2):
            place = z if t == 0 else nz - 1 - z

            @pl.when(place < nz - 1)
            def _(t=t):
                chain_copy(t, c).wait_send()
        return 0
    lax.fori_loop(0, chunks, drain, 0)


PLAN = ((1, 2, 3, 4), (4, 4, 4), (4, 4, 2, 0))


def run_state(u, chain, suf, pre, eb, ex, nz, nrow, nx, plan=PLAN):
    heads = nz * GH
    chunks = heads // HC
    cut = E // nrow
    half = nz // 2
    vm = pl.BlockSpec(memory_space=pltpu.VMEM)
    dma = pltpu.SemaphoreType.DMA
    return pl.pallas_call(
        functools.partial(state_kernel, nz, nrow, nx, plan),
        out_shape=jax.ShapeDtypeStruct((2, heads, E, E), BF16),
        in_specs=[vm] * 6,
        out_specs=vm,
        scratch_shapes=[
            pltpu.VMEM((2, 2, half, GH, E, E), BF16),
            pltpu.VMEM((2, 2, half, GH, E, E), BF16),
            pltpu.VMEM((2, GH, E, E), BF16),
            pltpu.VMEM((nrow, 2, GH, cut, E), BF16),
            pltpu.VMEM((2, GH, cut, E), BF16),
            pltpu.VMEM((nx, 2, GH, cut, E), BF16),
            pltpu.VMEM((nrow, 2, GH, cut, E), BF16),
            pltpu.VMEM((nz, 2, GH, E, E), BF16),
            pltpu.VMEM((2, heads, E, E), BF16),
            pltpu.VMEM((2, heads, E, E), BF16),
            dma((2, 2, half)), dma((2, 2, half)),
            dma((nrow - 1,)), dma,
            dma((nx - 1,)), dma,
            dma((nrow - 1,)), dma,
            dma((2, 2, half)), dma((2, 2, half)),
            dma((2, chunks)), dma((2, chunks)),
        ],
        compiler_params=pltpu.CompilerParams(collective_id=2, has_side_effects=True),
        name="state_scan",
    )(u, chain[:, None], suf[:, None], pre[:, None], eb, ex)


def on_device(nz, nrow, nx, q, k, v, g, decay):
    heads = nz * GH
    dz, lb, lx = run_decay(decay, nz, nrow, nx)
    run, start, block, end = (dz[:, i * GH:(i + 1) * GH].reshape(heads, E) for i in range(4))
    r = run - start
    c = end - start
    chain = jnp.exp(-c)
    suf = jnp.exp(end - block)
    pre = jnp.exp(-start)
    u = run_update(q, k, v, g, r, c)
    states = run_state(u, chain, suf, pre, jnp.exp(-lb), jnp.exp(-lx), nz, nrow, nx)
    return run_output(q, k, v, g, r, c, states)


def solution(mesh):
    nz = mesh.shape["head"]
    nrow = ROWS
    nx = mesh.shape["seq"] // nrow
    tok = P(("seq", "head"), None)
    return jax.shard_map(
        functools.partial(on_device, nz, nrow, nx), mesh=mesh,
        in_specs=(tok, tok, tok, tok, P("head", "seq")),
        out_specs=(tok,) * 4, check_vma=False)
```

```python
import functools

import jax
import jax.numpy as jnp
from jax import lax
from jax.experimental import pallas as pl
from jax.experimental.pallas import tpu as pltpu
from jax.sharding import PartitionSpec as P

E = 128
SCALE = E ** -0.5
GH = 4
HC = 2
LAG = 2
ROWS = 8
MESH = pl.DeviceIdType.MESH
F32 = jnp.float32
BF16 = jnp.bfloat16


def total_wait(ref, count, sem):
    part = ref.at[pl.ds(0, count)]
    pltpu.make_async_copy(part, part, sem).wait()


def barrier_with(peers):
    barrier = pltpu.get_barrier_semaphore()
    for peer in peers:
        pl.semaphore_signal(barrier, inc=1, device_id=peer, device_id_type=MESH)
    pl.semaphore_wait(barrier, len(peers))


def column_of(row):
    return jnp.transpose(jnp.broadcast_to(row, (E, E)))


def tdot(a, b):
    return lax.dot_general(a, b, (((0,), (0,)), ((), ())), preferred_element_type=F32)


def ntdot(a, b):
    return lax.dot_general(a, b, (((1,), (1,)), ((), ())), preferred_element_type=F32)


def dot(a, b):
    return jnp.dot(a, b, preferred_element_type=F32)


def state_kernel(nz, nrow, nx, plan, q_ref, k_ref, v_ref, g_ref, decay_ref,
                 out_ref, sc_ref, rc_ref,
                 msg, dz, bl, lb, rs, lx, eb, ex, fac, u,
                 rs_in, rs_out, tot, ta, rxo, rx, so, sa, ch_in, ch_out,
                 dz_s, dz_r, lb_s, lb_r, lx_s, lx_r,
                 rs_s, rs_r, ta_s, ta_r, rx_s, rx_r, so_s, so_r, ag_s, ag_r, ch_s, ch_r):
    z = lax.axis_index("head")
    sq = lax.axis_index("seq")
    x = sq // nrow
    m = sq % nrow
    right = (z + 1) % nz
    left = (z + nz - 1) % nz
    heads = nz * GH
    chunks = heads // HC
    cut = E // nrow
    toward = ((sq, right), (sq, left))
    z_peers = [(z + i) % nz for i in range(1, nz)]
    m_peers = [(m + i) % nrow for i in range(1, nrow)]
    x_peers = [(x + i) % nx for i in range(1, nx)]
    barrier_with([(sq, p) for p in z_peers] + [(x * nrow + p, z) for p in m_peers]
                 + [(p * nrow + m, z) for p in x_peers])
    pending = []

    run = decay_ref[...]
    length = run.shape[1]
    lane = lax.broadcasted_iota(jnp.int32, run.shape, 1)
    shift = 1
    while shift < length:
        run = run + jnp.where(lane >= shift, pltpu.roll(run, shift, 1), 0.0)
        shift *= 2
    block_log = jnp.broadcast_to(run[:, length - 1:], (GH, E))
    start = jnp.zeros((GH, E), F32)
    for p in range(nz):
        part = run[:, p * E:(p + 1) * E]
        end = jnp.broadcast_to(part[:, E - 1:], (GH, E))
        msg[p, 0:GH, :] = part - start
        msg[p, GH:2 * GH, :] = start
        msg[p, 2 * GH:3 * GH, :] = block_log - end
        msg[p, 3 * GH:, :] = end - start
        start = end
    bl[0:GH, :] = block_log
    bl[GH:, :] = jnp.zeros((8 - GH, E), F32)
    for i, p in enumerate(z_peers):
        pending.append(pltpu.make_async_remote_copy(
            msg.at[p], dz.at[z], dz_s.at[i], dz_r, device_id=(sq, p), device_id_type=MESH))
        pending[-1].start()
    for i, p in enumerate(m_peers):
        pending.append(pltpu.make_async_remote_copy(
            bl, lb.at[m], lb_s.at[i], lb_r, device_id=(x * nrow + p, z), device_id_type=MESH))
        pending[-1].start()
    dz[pl.ds(z, 1)] = msg[pl.ds(z, 1)]
    lb[pl.ds(m, 1)] = bl[...][None]

    def hops(way, t):
        return nz // 2 if way == t else nz // 2 - 1

    def sign(way):
        return 1 if way == 0 else -1

    for t in range(2):
        place = z if t == 0 else nz - 1 - z

        @pl.when(place == 0)
        def _(t=t):
            def clear(h, _):
                ch_in[t, h] = jnp.zeros((E, E), BF16)
                return 0
            lax.fori_loop(0, heads, clear, 0)

    total_wait(dz, nz - 1, dz_r)
    for p in range(nz):
        for i in range(GH):
            rc_ref[p * GH + i, 0:1, :] = dz[p, i:i + 1, :]
            rc_ref[p * GH + i, 1:2, :] = dz[p, 3 * GH + i:3 * GH + i + 1, :]
            fac[p * GH + i, 0:1, :] = jnp.exp(-dz[p, GH + i:GH + i + 1, :])
            fac[p * GH + i, 1:2, :] = jnp.exp(-dz[p, 2 * GH + i:2 * GH + i + 1, :])
            fac[p * GH + i, 2:3, :] = jnp.exp(-dz[p, 3 * GH + i:3 * GH + i + 1, :])

    def before(t, h):
        return fac[h, 1 - t:2 - t, :]

    def after(t, h):
        return fac[h, t:t + 1, :]

    done = set()

    def update_group(off):
        off %= nz
        if off in done:
            return
        done.add(off)
        group = (z + off) % nz

        def one(i, _):
            h = group * GH + i
            cols = pl.ds(pl.multiple_of(h * E, E), E)
            r_col = column_of(rc_ref[h, 0:1, :])
            keyed = (k_ref[:, cols].astype(F32) * jnp.exp(r_col - rc_ref[h, 1:2, :])).astype(BF16)
            queried = (q_ref[:, cols].astype(F32) * jnp.exp(-r_col)).astype(BF16)
            u[0, h] = tdot(keyed, v_ref[:, cols]).astype(BF16)
            u[1, h] = (SCALE * tdot(queried, g_ref[:, cols])).astype(BF16)
            return 0
        lax.fori_loop(0, GH, one, 0, unroll=True)

    filled = [0]

    def fill_run(count):
        count = min(count, heads - filled[0])
        if count <= 0:
            return
        causal = (lax.broadcasted_iota(jnp.int32, (E, E), 0) >= lax.broadcasted_iota(jnp.int32, (E, E), 1))

        def one(h, _):
            cols = pl.ds(pl.multiple_of(h * E, E), E)
            r_row = rc_ref[h, 0:1, :]
            r_col = column_of(r_row)
            mask = jnp.where(causal, jnp.exp(jnp.where(causal, r_row - r_col, 0.0)), 0.0) * SCALE
            sc_ref[0, h] = (ntdot(q_ref[:, cols], k_ref[:, cols]) * mask).astype(BF16)
            sc_ref[1, h] = (ntdot(g_ref[:, cols], v_ref[:, cols]) * mask).astype(BF16)
            return 0
        lax.fori_loop(filled[0], filled[0] + count, one, 0)
        filled[0] += count

    def chain_copy(t, c):
        part = pl.ds(c * HC, HC)
        return pltpu.make_async_remote_copy(
            ch_out.at[t, part], ch_in.at[t, part], ch_s.at[t, c], ch_r.at[t, c],
            device_id=toward[t], device_id_type=MESH)

    def chain_step(step, _):
        for t in range(2):
            place = z if t == 0 else nz - 1 - z
            c = step - LAG * place

            @pl.when((c >= 0) & (c < chunks))
            def _(t=t, place=place, c=c):
                @pl.when(place > 0)
                def _():
                    chain_copy(t, c).wait_recv()

                @pl.when(place < nz - 1)
                def _():
                    for i in range(HC):
                        h = c * HC + i
                        nxt = fac[h, 2:3, :] * ch_in[t, h].astype(F32) + u[t, h].astype(F32)
                        ch_out[t, h] = nxt.astype(BF16)
                    chain_copy(t, c).start()
        return 0

    chain_at = [0]
    chain_all = chunks + LAG * (nz - 1)

    def chain_run(count):
        count = min(count, chain_all - chain_at[0])
        if count > 0:
            lax.fori_loop(chain_at[0], chain_at[0] + count, chain_step, 0)
            chain_at[0] += count

    def spare(point):
        chain_run(plan[point][0])
        fill_run(plan[point][1])

    def rs_copy(way, t, s):
        return pltpu.make_async_remote_copy(
            rs_out.at[way, t, s], rs_in.at[way, t, s], rs_s.at[way, t, s], rs_r.at[way, t, s],
            device_id=toward[way], device_id_type=MESH)

    for s in range(nz // 2):
        for way, t in ((0, 0), (1, 1), (0, 1), (1, 0)):
            k = hops(way, t)
            if s >= k:
                continue
            off = sign(way) * (k - s)
            update_group(off)
            group = (z + off + nz) % nz
            if s > 0:
                rs_copy(way, t, s - 1).wait_recv()

            def fold(i, _, way=way, t=t, s=s, group=group):
                h = group * GH + i
                val = before(t, h) * u[t, h].astype(F32)
                if s > 0:
                    val = val + rs_in[way, t, s - 1, i].astype(F32)
                rs_out[way, t, s, i] = val.astype(BF16)
                return 0
            lax.fori_loop(0, GH, fold, 0)
            pending.append(rs_copy(way, t, s))
            pending[-1].start()
            if s > 0:
                chain_run(plan[s][0])
        if s == 0:
            for off in range(nz // 2, -1, -1):
                update_group(off)
                update_group(-off)
            total_wait(lb, nrow - 1, lb_r)
            rs[...] = jnp.sum(lb[...], axis=0)
            eb[...] = jnp.exp(-lb[...])
            for i, p in enumerate(x_peers):
                pending.append(pltpu.make_async_remote_copy(
                    rs, lx.at[x], lx_s.at[i], lx_r, device_id=(p * nrow + m, z), device_id_type=MESH))
                pending[-1].start()
            lx[pl.ds(x, 1)] = rs[...][None]
        fill_run(plan[s][1])
    for t in range(2):
        for way in range(2):
            rs_copy(way, t, hops(way, t) - 1).wait_recv()

        def finish(i, _, t=t):
            h = z * GH + i
            val = before(t, h) * u[t, h].astype(F32)
            for way in range(2):
                val = val + rs_in[way, t, hops(way, t) - 1, i].astype(F32)
            tot[t, i] = val.astype(BF16)
            return 0
        lax.fori_loop(0, GH, finish, 0)

    for i, p in enumerate(m_peers):
        copy = pltpu.make_async_remote_copy(
            tot.at[:, :, pl.ds(p * cut, cut), :], ta.at[m], ta_s.at[i], ta_r,
            device_id=(x * nrow + p, z), device_id_type=MESH)
        copy.start()
        pending.append(copy)
    ta[pl.ds(m, 1)] = tot[:, :, pl.ds(pl.multiple_of(m * cut, cut), cut), :][None]
    total_wait(lx, nx - 1, lx_r)
    ex[...] = jnp.exp(-lx[...])
    spare(nz // 2)
    total_wait(ta, nrow - 1, ta_r)
    order = (list(range(nrow)), list(range(nrow))[::-1])
    for t in range(2):
        for i in range(GH):
            acc = ta[order[t][0], t, i].astype(F32)
            for b in order[t][1:]:
                acc = eb[b, i:i + 1, :] * acc + ta[b, t, i].astype(F32)
            rxo[t, i] = acc.astype(BF16)
    for i, p in enumerate(x_peers):
        copy = pltpu.make_async_remote_copy(
            rxo, rx.at[x], rx_s.at[i], rx_r, device_id=(p * nrow + m, z), device_id_type=MESH)
        copy.start()
        pending.append(copy)
    rx[pl.ds(x, 1)] = rxo[...][None]
    spare(nz // 2 + 1)
    total_wait(rx, nx - 1, rx_r)
    for t in range(2):
        for i in range(GH):
            acc = jnp.zeros((cut, E), F32)
            for b in (range(nx) if t == 0 else range(nx - 1, -1, -1)):
                use = (b < x) if t == 0 else (b > x)
                new = ex[b, i:i + 1, :] * acc + rx[b, t, i].astype(F32)
                acc = jnp.where(use, new, acc)
            for b in order[t]:
                so[b, t, i] = acc.astype(BF16)
                acc = eb[b, i:i + 1, :] * acc + ta[b, t, i].astype(F32)
    rows = pl.ds(pl.multiple_of(m * cut, cut), cut)
    for i, p in enumerate(m_peers):
        copy = pltpu.make_async_remote_copy(
            so.at[p], sa.at[z, :, :, rows, :], so_s.at[i], so_r,
            device_id=(x * nrow + p, z), device_id_type=MESH)
        copy.start()
        pending.append(copy)
    sa[pl.ds(z, 1), :, :, rows, :] = so[pl.ds(m, 1)]
    spare(nz // 2 + 2)
    total_wait(so, nrow - 1, so_r)

    def ag_copy(way, t, s):
        group = (z - sign(way) * s + nz) % nz
        return pltpu.make_async_remote_copy(
            sa.at[group, t], sa.at[group, t], ag_s.at[way, t, s], ag_r.at[way, t, s],
            device_id=toward[way], device_id_type=MESH)

    def ag_wait(way, t, s):
        group = (z - sign(way) * (s + 1) + 2 * nz) % nz
        pltpu.make_async_remote_copy(
            sa.at[group, t], sa.at[group, t], ag_s.at[way, t, s], ag_r.at[way, t, s],
            device_id=toward[way], device_id_type=MESH).wait_recv()

    for s in range(nz // 2):
        for t in range(2):
            for way in range(2):
                if s >= hops(way, t):
                    continue
                if s > 0:
                    ag_wait(way, t, s - 1)
                pending.append(ag_copy(way, t, s))
                pending[-1].start()
                chain_run(plan[nz // 2 + 3 + s][0])
        fill_run(plan[nz // 2 + 3 + s][1])
    chain_run(chain_all)
    fill_run(heads)
    for t in range(2):
        for way in range(2):
            ag_wait(way, t, hops(way, t) - 1)

        def combine(h, _, t=t):
            val = after(t, h) * sa[h // GH, t, h % GH].astype(F32) + ch_in[t, h].astype(F32)
            out_ref[t, h] = val.astype(BF16)
            return 0
        lax.fori_loop(0, heads, combine, 0)

    for copy in pending:
        copy.wait_send()

    def drain(c, _):
        for t in range(2):
            place = z if t == 0 else nz - 1 - z

            @pl.when(place < nz - 1)
            def _(t=t):
                chain_copy(t, c).wait_send()
        return 0
    lax.fori_loop(0, chunks, drain, 0)


PLAN = ((0, 0), (1, 0), (1, 0), (1, 0), (3, 6), (3, 6), (3, 6), (1, 4), (1, 4), (1, 3), (1, 3))


def run_state(q, k, v, g, decay, nz, nrow, nx):
    heads = nz * GH
    chunks = heads // HC
    cut = E // nrow
    half = nz // 2
    vm = pl.BlockSpec(memory_space=pltpu.VMEM)
    dma = pltpu.SemaphoreType.DMA
    return pl.pallas_call(
        functools.partial(state_kernel, nz, nrow, nx, PLAN),
        out_shape=(jax.ShapeDtypeStruct((2, heads, E, E), BF16),
                   jax.ShapeDtypeStruct((2, heads, E, E), BF16),
                   jax.ShapeDtypeStruct((heads, 2, E), F32)),
        in_specs=[vm] * 5,
        out_specs=(vm, vm, vm),
        scratch_shapes=[
            pltpu.VMEM((nz, 4 * GH, E), F32), pltpu.VMEM((nz, 4 * GH, E), F32),
            pltpu.VMEM((8, E), F32), pltpu.VMEM((nrow, 8, E), F32),
            pltpu.VMEM((8, E), F32), pltpu.VMEM((nx, 8, E), F32),
            pltpu.VMEM((nrow, 8, E), F32), pltpu.VMEM((nx, 8, E), F32),
            pltpu.VMEM((heads, 8, E), F32),
            pltpu.VMEM((2, heads, E, E), BF16),
            pltpu.VMEM((2, 2, half, GH, E, E), BF16),
            pltpu.VMEM((2, 2, half, GH, E, E), BF16),
            pltpu.VMEM((2, GH, E, E), BF16),
            pltpu.VMEM((nrow, 2, GH, cut, E), BF16),
            pltpu.VMEM((2, GH, cut, E), BF16),
            pltpu.VMEM((nx, 2, GH, cut, E), BF16),
            pltpu.VMEM((nrow, 2, GH, cut, E), BF16),
            pltpu.VMEM((nz, 2, GH, E, E), BF16),
            pltpu.VMEM((2, heads, E, E), BF16),
            pltpu.VMEM((2, heads, E, E), BF16),
            dma((nz - 1,)), dma, dma((nrow - 1,)), dma, dma((nx - 1,)), dma,
            dma((2, 2, half)), dma((2, 2, half)),
            dma((nrow - 1,)), dma,
            dma((nx - 1,)), dma,
            dma((nrow - 1,)), dma,
            dma((2, 2, half)), dma((2, 2, half)),
            dma((2, chunks)), dma((2, chunks)),
        ],
        compiler_params=pltpu.CompilerParams(collective_id=1, has_side_effects=True),
        name="state_scan",
    )(q, k, v, g, decay)


def output_kernel(heads, q_ref, k_ref, v_ref, g_ref, rc_ref, s_ref, sc_ref, a_ref, dq_ref, dk_ref, dv_ref):
    for i in range(heads):
        cols = pl.ds(i * E, E)
        q, k, v, g = q_ref[:, cols], k_ref[:, cols], v_ref[:, cols], g_ref[:, cols]
        r_col = column_of(rc_ref[i, 0:1, :])
        growth = SCALE * jnp.exp(-r_col)
        weight = jnp.exp(r_col - rc_ref[i, 1:2, :])
        scores, grads = sc_ref[0, i], sc_ref[1, i]
        state, back = s_ref[0, i], s_ref[1, i]
        a_ref[:, cols] = (dot(scores, v) + growth * dot(q, state)).astype(BF16)
        dq_ref[:, cols] = (dot(grads, k) + growth * ntdot(g, state)).astype(BF16)
        dk_ref[:, cols] = (tdot(grads, q) + weight * ntdot(v, back)).astype(BF16)
        dv_ref[:, cols] = (tdot(scores, g) + weight * dot(k, back)).astype(BF16)


def run_output(q, k, v, g, rc, states, scores, heads=4):
    n = rc.shape[0]
    tok = pl.BlockSpec((E, heads * E), lambda i: (0, i))
    mat = pl.BlockSpec((2, heads, E, E), lambda i: (0, i, 0, 0))
    return pl.pallas_call(
        functools.partial(output_kernel, heads),
        grid=(n // heads,),
        out_shape=(jax.ShapeDtypeStruct(q.shape, BF16),) * 4,
        in_specs=[tok, tok, tok, tok, pl.BlockSpec((heads, 2, E), lambda i: (i, 0, 0)), mat, mat],
        out_specs=(tok, tok, tok, tok),
        name="chunk_outputs",
    )(q, k, v, g, rc, states, scores)


def on_device(nz, nrow, nx, q, k, v, g, decay):
    states, scores, rc = run_state(q, k, v, g, decay, nz, nrow, nx)
    return run_output(q, k, v, g, rc, states, scores)


def solution(mesh):
    nz = mesh.shape["head"]
    nrow = ROWS
    nx = mesh.shape["seq"] // nrow
    tok = P(("seq", "head"), None)
    return jax.shard_map(
        functools.partial(on_device, nz, nrow, nx), mesh=mesh,
        in_specs=(tok, tok, tok, tok, P("head", "seq")),
        out_specs=(tok,) * 4, check_vma=False)
```

```python
import functools

import jax
import jax.numpy as jnp
from jax import lax
from jax.experimental import pallas as pl
from jax.experimental.pallas import tpu as pltpu
from jax.sharding import PartitionSpec as P

E = 128
SCALE = E ** -0.5
GH = 4
HC = 2
LAG = 3
MIDDLE = 8
MESH = pl.DeviceIdType.MESH
F32 = jnp.float32
BF16 = jnp.bfloat16


def total_wait(ref, count, sem):
    part = ref.at[pl.ds(0, count)]
    pltpu.make_async_copy(part, part, sem).wait()


def barrier_with(peers):
    barrier = pltpu.get_barrier_semaphore()
    for peer in peers:
        pl.semaphore_signal(barrier, inc=1, device_id=peer, device_id_type=MESH)
    pl.semaphore_wait(barrier, len(peers))


def column_of(row):
    return jnp.transpose(jnp.broadcast_to(row, (E, E)))


def tdot(a, b):
    return lax.dot_general(a, b, (((0,), (0,)), ((), ())), preferred_element_type=F32)


def ntdot(a, b):
    return lax.dot_general(a, b, (((1,), (1,)), ((), ())), preferred_element_type=F32)


def dot(a, b):
    return jnp.dot(a, b, preferred_element_type=F32)


def state_kernel(nz, nseq, q_ref, k_ref, v_ref, g_ref, decay_ref,
                 out_ref, sc_ref, rc_ref,
                 msg, dz, bl, lb, eb, fac, u, tot, ta, so, sa, ch_in, ch_out,
                 dz_s, dz_r, lb_s, lb_r, tt_r, ta_s, ta_r, so_s, so_r, ag_s, ag_r, ch_s, ch_r):
    z = lax.axis_index("head")
    sq = lax.axis_index("seq")
    right = (z + 1) % nz
    left = (z + nz - 1) % nz
    heads = nz * GH
    chunks = heads // HC
    waves = chunks // nz
    members = nseq // 2
    cut = HC * E // members
    per = E // cut
    toward = ((sq, right), (sq, left))
    z_peers = [(z + i) % nz for i in range(1, nz)]
    s_peers = [(sq + i) % nseq for i in range(1, nseq)]
    barrier_with([(sq, p) for p in z_peers] + [(p, z) for p in s_peers])
    pending = []

    run = decay_ref[...]
    length = run.shape[1]
    lane = lax.broadcasted_iota(jnp.int32, run.shape, 1)
    shift = 1
    while shift < length:
        run = run + jnp.where(lane >= shift, pltpu.roll(run, shift, 1), 0.0)
        shift *= 2
    block_log = jnp.broadcast_to(run[:, length - 1:], (GH, E))
    start = jnp.zeros((GH, E), F32)
    for p in range(nz):
        part = run[:, p * E:(p + 1) * E]
        end = jnp.broadcast_to(part[:, E - 1:], (GH, E))
        msg[p, 0:GH, :] = part - start
        msg[p, GH:2 * GH, :] = start
        msg[p, 2 * GH:3 * GH, :] = block_log - end
        msg[p, 3 * GH:, :] = end - start
        start = end
    for i, p in enumerate(z_peers):
        pending.append(pltpu.make_async_remote_copy(
            msg.at[p], dz.at[z], dz_s.at[i], dz_r, device_id=(sq, p), device_id_type=MESH))
        pending[-1].start()
    dz[pl.ds(z, 1)] = msg[pl.ds(z, 1)]

    def hops(way, t):
        return nz // 2 if way == t else nz // 2 - 1

    def sign(way):
        return 1 if way == 0 else -1

    for t in range(2):
        place = z if t == 0 else nz - 1 - z

        @pl.when(place == 0)
        def _(t=t):
            def clear(h, _):
                ch_in[t, h] = jnp.zeros((E, E), BF16)
                return 0
            lax.fori_loop(0, heads, clear, 0)

    total_wait(dz, nz - 1, dz_r)
    for p in range(nz):
        for i in range(GH):
            start, rest, own = (dz[p, n * GH + i:n * GH + i + 1, :] for n in range(1, 4))
            rc_ref[p * GH + i, 0:1, :] = dz[p, i:i + 1, :]
            rc_ref[p * GH + i, 1:2, :] = own
            fac[p * GH + i, 0:1, :] = jnp.exp(-start)
            fac[p * GH + i, 1:2, :] = jnp.exp(-rest)
            fac[p * GH + i, 2:3, :] = jnp.exp(-own)
            fac[p * GH + i, 3:4, :] = start + rest + own

    def after(t, h):
        return fac[h, t:t + 1, :]

    def lb_copy(i):
        p = (sq + i) % nseq
        return pltpu.make_async_remote_copy(
            bl, lb.at[sq], lb_s.at[i], lb_r, device_id=(p, z), device_id_type=MESH)

    def send_logs():
        bl[...] = jnp.zeros((8, E), F32)
        for w in range(waves):
            for i in range(HC):
                bl[w * HC + i:w * HC + i + 1, :] = fac[(w * nz + z) * HC + i, 3:4, :]

        def one(i, _):
            lb_copy(i).start()
            return 0
        lax.fori_loop(1, nseq, one, 0)
        lb[pl.ds(sq, 1)] = bl[...][None]

    def fill(h):
        causal = (lax.broadcasted_iota(jnp.int32, (E, E), 0) >= lax.broadcasted_iota(jnp.int32, (E, E), 1))
        cols = pl.ds(pl.multiple_of(h * E, E), E)
        r_row = rc_ref[h, 0:1, :]
        r_col = column_of(r_row)
        mask = jnp.where(causal, jnp.exp(jnp.where(causal, r_row - r_col, 0.0)), 0.0) * SCALE
        sc_ref[0, h] = (ntdot(q_ref[:, cols], k_ref[:, cols]) * mask).astype(BF16)
        sc_ref[1, h] = (ntdot(g_ref[:, cols], v_ref[:, cols]) * mask).astype(BF16)

    def place_of(t):
        return z if t == 0 else nz - 1 - z

    def chain_copy(t, c):
        part = pl.ds(c * HC, HC)
        return pltpu.make_async_remote_copy(
            ch_out.at[t, part], ch_in.at[t, part], ch_s.at[t, c], ch_r.at[t, c],
            device_id=toward[t], device_id_type=MESH)

    def total_copy(t, c):
        w = c // nz
        return pltpu.make_async_remote_copy(
            ch_out.at[t, pl.ds(c * HC, HC)], tot.at[w, t], ch_s.at[t, c], tt_r.at[w, t],
            device_id=(sq, c % nz), device_id_type=MESH)

    def prepare(step):
        for t in range(2):
            c = step - LAG * place_of(t)

            @pl.when((c >= 0) & (c < chunks))
            def _(t=t, c=c):
                for i in range(HC):
                    h = c * HC + i
                    cols = pl.ds(pl.multiple_of(h * E, E), E)
                    r_col = column_of(rc_ref[h, 0:1, :])
                    if t == 0:
                        keyed = (k_ref[:, cols].astype(F32) * jnp.exp(r_col - rc_ref[h, 1:2, :])).astype(BF16)
                        u[step % 2, t, i] = tdot(keyed, v_ref[:, cols])
                    else:
                        queried = (q_ref[:, cols].astype(F32) * jnp.exp(-r_col)).astype(BF16)
                        u[step % 2, t, i] = SCALE * tdot(queried, g_ref[:, cols])

    def chain_step(step, _):
        for t in range(2):
            place = place_of(t)
            c = step - LAG * place

            @pl.when((c >= 0) & (c < chunks))
            def _(t=t, place=place, c=c):
                @pl.when(place > 0)
                def _():
                    chain_copy(t, c).wait_recv()
                for i in range(HC):
                    h = c * HC + i
                    ch_out[t, h] = (fac[h, 2:3, :] * ch_in[t, h].astype(F32) + u[step % 2, t, i]).astype(BF16)

                @pl.when(place < nz - 1)
                def _():
                    chain_copy(t, c).start()

                @pl.when((place == nz - 1) & (c % nz != z))
                def _():
                    total_copy(t, c).start()

                @pl.when((place == nz - 1) & (c % nz == z))
                def _():
                    tot[c // nz, t] = ch_out[t, pl.ds(c * HC, HC)]
        prepare(step + 1)

        @pl.when(step < heads)
        def _():
            fill(step)
        return 0

    chain_at = [0]
    chain_all = chunks + LAG * (nz - 1)

    def chain_run(count):
        count = min(count, chain_all - chain_at[0])
        if count > 0:
            lax.fori_loop(chain_at[0], chain_at[0] + count, chain_step, 0)
            chain_at[0] += count

    my_t = sq // members
    my_j = sq % members

    def rows_of(j):
        return pl.ds(pl.multiple_of((j % per) * cut, cut), cut)

    def ta_copy(w, t, j):
        p = t * members + j
        return pltpu.make_async_remote_copy(
            tot.at[w, t, j // per, rows_of(j), :], ta.at[w, sq], ta_s.at[w, p], ta_r.at[w],
            device_id=(p, z), device_id_type=MESH)

    def send_totals(w):
        for t in range(2):
            @pl.when(place_of(t) != nz - 1)
            def _(t=t):
                pltpu.make_async_remote_copy(
                    tot.at[w, t], tot.at[w, t], tt_r.at[w, t], tt_r.at[w, t],
                    device_id=toward[t], device_id_type=MESH).wait_recv()

            def send(j, _, t=t):
                @pl.when(t * members + j != sq)
                def _():
                    ta_copy(w, t, j).start()

                @pl.when(t * members + j == sq)
                def _():
                    ta[w, sq] = tot[w, t, j // per, rows_of(j), :]
                return 0
            lax.fori_loop(0, members, send, 0)

    def so_copy(w, p):
        return pltpu.make_async_remote_copy(
            so.at[w, p], sa.at[w, z, my_t, my_j // per, rows_of(my_j), :], so_s.at[w, p], so_r.at[w, my_t],
            device_id=(p, z), device_id_type=MESH)

    def scan_blocks(w):
        total_wait(ta.at[w], nseq - 1, ta_r.at[w])

        def one(n, acc):
            b = n + my_t * (nseq - 1 - 2 * n)
            so[w, b] = acc.astype(BF16)
            return eb[b, pl.ds(w * HC + my_j // per, 1), :] * acc + ta[w, b].astype(F32)
        lax.fori_loop(0, nseq, one, jnp.zeros((cut, E), F32), unroll=4)

        def send(i, _):
            so_copy(w, (sq + i) % nseq).start()
            return 0
        lax.fori_loop(1, nseq, send, 0)
        sa[w, z, my_t, my_j // per, rows_of(my_j), :] = so[w, sq]

    def so_wait(w, t):
        @pl.when(my_t == t)
        def _():
            total_wait(so.at[w], members - 1, so_r.at[w, t])

        @pl.when(my_t != t)
        def _():
            total_wait(so.at[w], members, so_r.at[w, t])

    def ag_copy(w, way, t, s):
        group = (z - sign(way) * s + nz) % nz
        return pltpu.make_async_remote_copy(
            sa.at[w, group, t], sa.at[w, group, t], ag_s.at[w, way, t, s], ag_r.at[w, way, t, s],
            device_id=toward[way], device_id_type=MESH)

    def ag_wait(w, way, t, s):
        group = (z - sign(way) * (s + 1) + 2 * nz) % nz
        pltpu.make_async_remote_copy(
            sa.at[w, group, t], sa.at[w, group, t], ag_s.at[w, way, t, s], ag_r.at[w, way, t, s],
            device_id=toward[way], device_id_type=MESH).wait_recv()

    def ag_hop(w, s):
        for t in range(2):
            if s == 0:
                so_wait(w, t)
            for way in range(2):
                if s >= hops(way, t):
                    continue
                if s > 0:
                    ag_wait(w, way, t, s - 1)
                pending.append(ag_copy(w, way, t, s))
                pending[-1].start()

    def combine(w, t, off):
        group = (z + off + nz) % nz
        for i in range(HC):
            h = (w * nz + group) * HC + i
            val = after(t, h) * sa[w, group, t, i].astype(F32) + ch_in[t, h].astype(F32)
            out_ref[t, h] = val.astype(BF16)

    def combine_early(w):
        for t in range(2):
            for off in range(t + 1 - nz // 2, nz // 2 - 1 + t):
                combine(w, t, off)

    def combine_last(w):
        for way, t in ((1, 0), (0, 1), (0, 0), (1, 1)):
            ag_wait(w, way, t, hops(way, t) - 1)
            combine(w, t, -sign(way) * hops(way, t))

    half = nz // 2
    prepare(0)
    chain_run(2)
    send_logs()
    chain_run(nz + LAG * (nz - 1) - 2)
    total_wait(lb, nseq - 1, lb_r)
    eb[...] = jnp.exp(-lb[...])
    send_totals(0)
    chain_run(MIDDLE)
    scan_blocks(0)
    chain_run(chain_all)
    send_totals(1)
    ag_hop(0, 0)
    if half > 2:
        ag_hop(0, 1)
    scan_blocks(1)
    for s in range(2, half - 1):
        ag_hop(0, s)
    ag_hop(1, 0)
    if half > 1:
        ag_hop(0, half - 1)
    combine_early(0)
    for s in range(1, half - 1):
        ag_hop(1, s)
    combine_last(0)
    if half > 1:
        ag_hop(1, half - 1)
    combine_early(1)
    combine_last(1)

    for copy in pending:
        copy.wait_send()

    def drain_peers(i, _):
        lb_copy(i).wait_send()
        for w in range(waves):
            so_copy(w, (sq + i) % nseq).wait_send()
        return 0
    lax.fori_loop(1, nseq, drain_peers, 0)

    def drain_totals(j, _):
        for w in range(waves):
            for t in range(2):
                @pl.when(t * members + j != sq)
                def _(w=w, t=t):
                    ta_copy(w, t, j).wait_send()
        return 0
    lax.fori_loop(0, members, drain_totals, 0)

    def drain_chain(c, _):
        for t in range(2):
            place = place_of(t)

            @pl.when((place < nz - 1) | (c % nz != z))
            def _(t=t):
                chain_copy(t, c).wait_send()
        return 0
    lax.fori_loop(0, chunks, drain_chain, 0)


def run_state(q, k, v, g, decay, nz, nseq):
    heads = nz * GH
    chunks = heads // HC
    waves = chunks // nz
    cut = 2 * HC * E // nseq
    half = nz // 2
    vm = pl.BlockSpec(memory_space=pltpu.VMEM)
    dma = pltpu.SemaphoreType.DMA
    return pl.pallas_call(
        functools.partial(state_kernel, nz, nseq),
        out_shape=(jax.ShapeDtypeStruct((2, heads, E, E), BF16),
                   jax.ShapeDtypeStruct((2, heads, E, E), BF16),
                   jax.ShapeDtypeStruct((heads, 2, E), F32)),
        in_specs=[vm] * 5,
        out_specs=(vm, vm, vm),
        scratch_shapes=[
            pltpu.VMEM((nz, 4 * GH, E), F32), pltpu.VMEM((nz, 4 * GH, E), F32),
            pltpu.VMEM((8, E), F32), pltpu.VMEM((nseq, 8, E), F32), pltpu.VMEM((nseq, 8, E), F32),
            pltpu.VMEM((heads, 8, E), F32),
            pltpu.VMEM((2, 2, HC, E, E), F32),
            pltpu.VMEM((waves, 2, HC, E, E), BF16),
            pltpu.VMEM((waves, nseq, cut, E), BF16),
            pltpu.VMEM((waves, nseq, cut, E), BF16),
            pltpu.VMEM((waves, nz, 2, HC, E, E), BF16),
            pltpu.VMEM((2, heads, E, E), BF16),
            pltpu.VMEM((2, heads, E, E), BF16),
            dma((nz - 1,)), dma, dma((nseq,)), dma, dma((waves, 2)),
            dma((waves, nseq)), dma((waves,)),
            dma((waves, nseq)), dma((waves, 2)),
            dma((waves, 2, 2, half)), dma((waves, 2, 2, half)),
            dma((2, chunks)), dma((2, chunks)),
        ],
        compiler_params=pltpu.CompilerParams(collective_id=1, has_side_effects=True),
        name="state_scan",
    )(q, k, v, g, decay)


def output_kernel(heads, q_ref, k_ref, v_ref, g_ref, rc_ref, s_ref, sc_ref, a_ref, dq_ref, dk_ref, dv_ref):
    for i in range(heads):
        cols = pl.ds(i * E, E)
        q, k, v, g = q_ref[:, cols], k_ref[:, cols], v_ref[:, cols], g_ref[:, cols]
        r_col = column_of(rc_ref[i, 0:1, :])
        growth = SCALE * jnp.exp(-r_col)
        weight = jnp.exp(r_col - rc_ref[i, 1:2, :])
        scores, grads = sc_ref[0, i], sc_ref[1, i]
        state, back = s_ref[0, i], s_ref[1, i]
        a_ref[:, cols] = (dot(scores, v) + growth * dot(q, state)).astype(BF16)
        dq_ref[:, cols] = (dot(grads, k) + growth * ntdot(g, state)).astype(BF16)
        dk_ref[:, cols] = (tdot(grads, q) + weight * ntdot(v, back)).astype(BF16)
        dv_ref[:, cols] = (tdot(scores, g) + weight * dot(k, back)).astype(BF16)


def run_output(q, k, v, g, rc, states, scores, heads=8):
    n = rc.shape[0]
    tok = pl.BlockSpec((E, heads * E), lambda i: (0, i))
    mat = pl.BlockSpec((2, heads, E, E), lambda i: (0, i, 0, 0))
    return pl.pallas_call(
        functools.partial(output_kernel, heads),
        grid=(n // heads,),
        out_shape=(jax.ShapeDtypeStruct(q.shape, BF16),) * 4,
        in_specs=[tok, tok, tok, tok, pl.BlockSpec((heads, 2, E), lambda i: (i, 0, 0)), mat, mat],
        out_specs=(tok, tok, tok, tok),
        name="chunk_outputs",
    )(q, k, v, g, rc, states, scores)


def on_device(nz, nseq, q, k, v, g, decay):
    states, scores, rc = run_state(q, k, v, g, decay, nz, nseq)
    return run_output(q, k, v, g, rc, states, scores)


def solution(mesh):
    nz = mesh.shape["head"]
    nseq = mesh.shape["seq"]
    tok = P(("seq", "head"), None)
    return jax.shard_map(
        functools.partial(on_device, nz, nseq), mesh=mesh,
        in_specs=(tok, tok, tok, tok, P("head", "seq")),
        out_specs=(tok,) * 4, check_vma=False)
```

```python
import functools

import jax
import jax.numpy as jnp
from jax import lax
from jax.experimental import pallas as pl
from jax.experimental.pallas import tpu as pltpu
from jax.sharding import PartitionSpec as P

E = 128
SCALE = E ** -0.5
GH = 4
HC = 2
LAG = 3
MIDDLE = 8
MESH = pl.DeviceIdType.MESH
F32 = jnp.float32
BF16 = jnp.bfloat16


def total_wait(ref, count, sem):
    part = ref.at[pl.ds(0, count)]
    pltpu.make_async_copy(part, part, sem).wait()


def barrier_with(peers):
    barrier = pltpu.get_barrier_semaphore()
    for peer in peers:
        pl.semaphore_signal(barrier, inc=1, device_id=peer, device_id_type=MESH)
    pl.semaphore_wait(barrier, len(peers))


def column_of(row):
    return jnp.transpose(jnp.broadcast_to(row, (E, E)))


def tdot(a, b):
    return lax.dot_general(a, b, (((0,), (0,)), ((), ())), preferred_element_type=F32)


def ntdot(a, b):
    return lax.dot_general(a, b, (((1,), (1,)), ((), ())), preferred_element_type=F32)


def dot(a, b):
    return jnp.dot(a, b, preferred_element_type=F32)


def state_kernel(nz, nseq, q_ref, k_ref, v_ref, g_ref, decay_ref,
                 out_ref, sc_ref, rc_ref,
                 msg, dz, bl, lb, eb, fac, u, tot, ta, so, sa, ch_in, ch_out,
                 dz_s, dz_r, lb_s, lb_r, tt_r, ta_s, ta_r, so_s, so_r, ag_s, ag_r, ch_s, ch_r):
    z = lax.axis_index("head")
    sq = lax.axis_index("seq")
    right = (z + 1) % nz
    left = (z + nz - 1) % nz
    heads = nz * GH
    chunks = heads // HC
    waves = chunks // nz
    members = nseq // 2
    cut = HC * E // members
    per = E // cut
    toward = ((sq, right), (sq, left))
    z_peers = [(z + i) % nz for i in range(1, nz)]
    s_peers = [(sq + i) % nseq for i in range(1, nseq)]
    barrier_with([(sq, p) for p in z_peers] + [(p, z) for p in s_peers])
    pending = []

    run = decay_ref[...]
    length = run.shape[1]
    lane = lax.broadcasted_iota(jnp.int32, run.shape, 1)
    shift = 1
    while shift < length:
        run = run + jnp.where(lane >= shift, pltpu.roll(run, shift, 1), 0.0)
        shift *= 2
    block_log = jnp.broadcast_to(run[:, length - 1:], (GH, E))
    start = jnp.zeros((GH, E), F32)
    for p in range(nz):
        part = run[:, p * E:(p + 1) * E]
        end = jnp.broadcast_to(part[:, E - 1:], (GH, E))
        msg[p, 0:GH, :] = part - start
        msg[p, GH:2 * GH, :] = start
        msg[p, 2 * GH:3 * GH, :] = block_log - end
        msg[p, 3 * GH:, :] = end - start
        start = end
    for i, p in enumerate(z_peers):
        pending.append(pltpu.make_async_remote_copy(
            msg.at[p], dz.at[z], dz_s.at[i], dz_r, device_id=(sq, p), device_id_type=MESH))
        pending[-1].start()
    dz[pl.ds(z, 1)] = msg[pl.ds(z, 1)]

    def hops(way, t):
        return nz // 2 if way == t else nz // 2 - 1

    def sign(way):
        return 1 if way == 0 else -1

    for t in range(2):
        place = z if t == 0 else nz - 1 - z

        @pl.when(place == 0)
        def _(t=t):
            def clear(h, _):
                ch_in[t, h] = jnp.zeros((E, E), BF16)
                return 0
            lax.fori_loop(0, heads, clear, 0)

    total_wait(dz, nz - 1, dz_r)
    for p in range(nz):
        for i in range(GH):
            start, rest, own = (dz[p, n * GH + i:n * GH + i + 1, :] for n in range(1, 4))
            rc_ref[p * GH + i, 0:1, :] = dz[p, i:i + 1, :]
            rc_ref[p * GH + i, 1:2, :] = own
            fac[p * GH + i, 0:1, :] = jnp.exp(-start)
            fac[p * GH + i, 1:2, :] = jnp.exp(-rest)
            fac[p * GH + i, 2:3, :] = jnp.exp(-own)
            fac[p * GH + i, 3:4, :] = start + rest + own

    def after(t, h):
        return fac[h, t:t + 1, :]

    def lb_copy(i):
        p = (sq + i) % nseq
        return pltpu.make_async_remote_copy(
            bl, lb.at[sq], lb_s.at[i], lb_r, device_id=(p, z), device_id_type=MESH)

    def send_logs():
        bl[...] = jnp.zeros((8, E), F32)
        for w in range(waves):
            for i in range(HC):
                bl[w * HC + i:w * HC + i + 1, :] = fac[(w * nz + z) * HC + i, 3:4, :]

        def one(i, _):
            lb_copy(i).start()
            return 0
        lax.fori_loop(1, nseq, one, 0)
        lb[pl.ds(sq, 1)] = bl[...][None]

    def fill(h):
        causal = (lax.broadcasted_iota(jnp.int32, (E, E), 0) >= lax.broadcasted_iota(jnp.int32, (E, E), 1))
        cols = pl.ds(pl.multiple_of(h * E, E), E)
        r_row = rc_ref[h, 0:1, :]
        r_col = column_of(r_row)
        mask = jnp.where(causal, jnp.exp(jnp.where(causal, r_row - r_col, 0.0)), 0.0) * SCALE
        sc_ref[0, h] = (ntdot(q_ref[:, cols], k_ref[:, cols]) * mask).astype(BF16)
        sc_ref[1, h] = (ntdot(g_ref[:, cols], v_ref[:, cols]) * mask).astype(BF16)

    def place_of(t):
        return z if t == 0 else nz - 1 - z

    def chain_copy(t, c):
        part = pl.ds(c * HC, HC)
        return pltpu.make_async_remote_copy(
            ch_out.at[t, part], ch_in.at[t, part], ch_s.at[t, c], ch_r.at[t, c],
            device_id=toward[t], device_id_type=MESH)

    def total_copy(t, c):
        w = c // nz
        return pltpu.make_async_remote_copy(
            ch_out.at[t, pl.ds(c * HC, HC)], tot.at[w, t], ch_s.at[t, c], tt_r.at[w, t],
            device_id=(sq, c % nz), device_id_type=MESH)

    def prepare(step):
        for t in range(2):
            c = step - LAG * place_of(t)

            @pl.when((c >= 0) & (c < chunks))
            def _(t=t, c=c):
                for i in range(HC):
                    h = c * HC + i
                    cols = pl.ds(pl.multiple_of(h * E, E), E)
                    r_col = column_of(rc_ref[h, 0:1, :])
                    if t == 0:
                        keyed = (k_ref[:, cols].astype(F32) * jnp.exp(r_col - rc_ref[h, 1:2, :])).astype(BF16)
                        u[step % 2, t, i] = tdot(keyed, v_ref[:, cols])
                    else:
                        queried = (q_ref[:, cols].astype(F32) * jnp.exp(-r_col)).astype(BF16)
                        u[step % 2, t, i] = SCALE * tdot(queried, g_ref[:, cols])

    def chain_step(step, _):
        for t in range(2):
            place = place_of(t)
            c = step - LAG * place

            @pl.when((c >= 0) & (c < chunks))
            def _(t=t, place=place, c=c):
                @pl.when(place > 0)
                def _():
                    chain_copy(t, c).wait_recv()
                for i in range(HC):
                    h = c * HC + i
                    ch_out[t, h] = (fac[h, 2:3, :] * ch_in[t, h].astype(F32) + u[step % 2, t, i]).astype(BF16)

                @pl.when(place < nz - 1)
                def _():
                    chain_copy(t, c).start()

                @pl.when((place == nz - 1) & (c % nz != z))
                def _():
                    total_copy(t, c).start()

                @pl.when((place == nz - 1) & (c % nz == z))
                def _():
                    tot[c // nz, t] = ch_out[t, pl.ds(c * HC, HC)]
        prepare(step + 1)

        @pl.when(step < heads)
        def _():
            fill(step)
        return 0

    chain_at = [0]
    chain_all = chunks + LAG * (nz - 1)

    def chain_run(count):
        count = min(count, chain_all - chain_at[0])
        if count > 0:
            lax.fori_loop(chain_at[0], chain_at[0] + count, chain_step, 0)
            chain_at[0] += count

    my_t = sq // members
    my_j = sq % members

    def rows_of(j):
        return pl.ds(pl.multiple_of((j % per) * cut, cut), cut)

    def ta_copy(w, t, j):
        p = t * members + j
        return pltpu.make_async_remote_copy(
            tot.at[w, t, j // per, rows_of(j), :], ta.at[w, sq], ta_s.at[w, p], ta_r.at[w],
            device_id=(p, z), device_id_type=MESH)

    def send_totals(w):
        for t in range(2):
            @pl.when(place_of(t) != nz - 1)
            def _(t=t):
                pltpu.make_async_remote_copy(
                    tot.at[w, t], tot.at[w, t], tt_r.at[w, t], tt_r.at[w, t],
                    device_id=toward[t], device_id_type=MESH).wait_recv()

            def send(j, _, t=t):
                @pl.when(t * members + j != sq)
                def _():
                    ta_copy(w, t, j).start()

                @pl.when(t * members + j == sq)
                def _():
                    ta[w, sq] = tot[w, t, j // per, rows_of(j), :]
                return 0
            lax.fori_loop(0, members, send, 0)

    def so_copy(w, p):
        return pltpu.make_async_remote_copy(
            so.at[w, p], sa.at[w, z, my_t, my_j // per, rows_of(my_j), :], so_s.at[w, p], so_r.at[w, my_t],
            device_id=(p, z), device_id_type=MESH)

    def scan_blocks(w):
        total_wait(ta.at[w], nseq - 1, ta_r.at[w])

        def one(n, acc):
            b = n + my_t * (nseq - 1 - 2 * n)
            so[w, b] = acc.astype(BF16)
            return eb[b, pl.ds(w * HC + my_j // per, 1), :] * acc + ta[w, b].astype(F32)
        lax.fori_loop(0, nseq, one, jnp.zeros((cut, E), F32), unroll=4)

        def send(i, _):
            so_copy(w, (sq + i) % nseq).start()
            return 0
        lax.fori_loop(1, nseq, send, 0)
        sa[w, z, my_t, my_j // per, rows_of(my_j), :] = so[w, sq]

    def so_wait(w, t):
        @pl.when(my_t == t)
        def _():
            total_wait(so.at[w], members - 1, so_r.at[w, t])

        @pl.when(my_t != t)
        def _():
            total_wait(so.at[w], members, so_r.at[w, t])

    def ag_copy(w, way, t, s):
        group = (z - sign(way) * s + nz) % nz
        return pltpu.make_async_remote_copy(
            sa.at[w, group, t], sa.at[w, group, t], ag_s.at[w, way, t, s], ag_r.at[w, way, t, s],
            device_id=toward[way], device_id_type=MESH)

    def ag_wait(w, way, t, s):
        group = (z - sign(way) * (s + 1) + 2 * nz) % nz
        pltpu.make_async_remote_copy(
            sa.at[w, group, t], sa.at[w, group, t], ag_s.at[w, way, t, s], ag_r.at[w, way, t, s],
            device_id=toward[way], device_id_type=MESH).wait_recv()

    def ag_hop(w, s):
        for t in range(2):
            if s == 0:
                so_wait(w, t)
            for way in range(2):
                if s >= hops(way, t):
                    continue
                if s > 0:
                    ag_wait(w, way, t, s - 1)
                pending.append(ag_copy(w, way, t, s))
                pending[-1].start()

    def combine(w, t, off):
        group = (z + off + nz) % nz
        for i in range(HC):
            h = (w * nz + group) * HC + i
            val = after(t, h) * sa[w, group, t, i].astype(F32) + ch_in[t, h].astype(F32)
            out_ref[t, h] = val.astype(BF16)

    def combine_early(w):
        for t in range(2):
            for off in range(t + 1 - nz // 2, nz // 2 - 1 + t):
                combine(w, t, off)

    def combine_last(w):
        for way, t in ((1, 0), (0, 1), (0, 0), (1, 1)):
            ag_wait(w, way, t, hops(way, t) - 1)
            combine(w, t, -sign(way) * hops(way, t))

    half = nz // 2
    prepare(0)
    chain_run(2)
    send_logs()
    chain_run(nz + LAG * (nz - 1) - 2)
    total_wait(lb, nseq - 1, lb_r)
    eb[...] = jnp.exp(-lb[...])
    send_totals(0)
    chain_run(MIDDLE)
    scan_blocks(0)
    chain_run(chain_all)
    send_totals(1)
    ag_hop(0, 0)
    if half > 2:
        ag_hop(0, 1)
    scan_blocks(1)
    for s in range(2, half - 1):
        ag_hop(0, s)
    ag_hop(1, 0)
    if half > 1:
        ag_hop(0, half - 1)
    for s in range(1, half - 1):
        ag_hop(1, s)
        combine_early(0) if s == 1 else None
    if half > 1:
        ag_hop(1, half - 1)
    combine_last(0)
    combine_early(1)
    combine_last(1)

    for copy in pending:
        copy.wait_send()

    def drain_peers(i, _):
        lb_copy(i).wait_send()
        for w in range(waves):
            so_copy(w, (sq + i) % nseq).wait_send()
        return 0
    lax.fori_loop(1, nseq, drain_peers, 0)

    def drain_totals(j, _):
        for w in range(waves):
            for t in range(2):
                @pl.when(t * members + j != sq)
                def _(w=w, t=t):
                    ta_copy(w, t, j).wait_send()
        return 0
    lax.fori_loop(0, members, drain_totals, 0)

    def drain_chain(c, _):
        for t in range(2):
            place = place_of(t)

            @pl.when((place < nz - 1) | (c % nz != z))
            def _(t=t):
                chain_copy(t, c).wait_send()
        return 0
    lax.fori_loop(0, chunks, drain_chain, 0)


def run_state(q, k, v, g, decay, nz, nseq):
    heads = nz * GH
    chunks = heads // HC
    waves = chunks // nz
    cut = 2 * HC * E // nseq
    half = nz // 2
    vm = pl.BlockSpec(memory_space=pltpu.VMEM)
    dma = pltpu.SemaphoreType.DMA
    return pl.pallas_call(
        functools.partial(state_kernel, nz, nseq),
        out_shape=(jax.ShapeDtypeStruct((2, heads, E, E), BF16),
                   jax.ShapeDtypeStruct((2, heads, E, E), BF16),
                   jax.ShapeDtypeStruct((heads, 2, E), F32)),
        in_specs=[vm] * 5,
        out_specs=(vm, vm, vm),
        scratch_shapes=[
            pltpu.VMEM((nz, 4 * GH, E), F32), pltpu.VMEM((nz, 4 * GH, E), F32),
            pltpu.VMEM((8, E), F32), pltpu.VMEM((nseq, 8, E), F32), pltpu.VMEM((nseq, 8, E), F32),
            pltpu.VMEM((heads, 8, E), F32),
            pltpu.VMEM((2, 2, HC, E, E), F32),
            pltpu.VMEM((waves, 2, HC, E, E), BF16),
            pltpu.VMEM((waves, nseq, cut, E), BF16),
            pltpu.VMEM((waves, nseq, cut, E), BF16),
            pltpu.VMEM((waves, nz, 2, HC, E, E), BF16),
            pltpu.VMEM((2, heads, E, E), BF16),
            pltpu.VMEM((2, heads, E, E), BF16),
            dma((nz - 1,)), dma, dma((nseq,)), dma, dma((waves, 2)),
            dma((waves, nseq)), dma((waves,)),
            dma((waves, nseq)), dma((waves, 2)),
            dma((waves, 2, 2, half)), dma((waves, 2, 2, half)),
            dma((2, chunks)), dma((2, chunks)),
        ],
        compiler_params=pltpu.CompilerParams(collective_id=1, has_side_effects=True),
        name="state_scan",
    )(q, k, v, g, decay)


def output_kernel(heads, q_ref, k_ref, v_ref, g_ref, rc_ref, s_ref, sc_ref, a_ref, dq_ref, dk_ref, dv_ref):
    for i in range(heads):
        cols = pl.ds(i * E, E)
        q, k, v, g = q_ref[:, cols], k_ref[:, cols], v_ref[:, cols], g_ref[:, cols]
        r_col = column_of(rc_ref[i, 0:1, :])
        growth = SCALE * jnp.exp(-r_col)
        weight = jnp.exp(r_col - rc_ref[i, 1:2, :])
        scores, grads = sc_ref[0, i], sc_ref[1, i]
        state, back = s_ref[0, i], s_ref[1, i]
        a_ref[:, cols] = (dot(scores, v) + growth * dot(q, state)).astype(BF16)
        dq_ref[:, cols] = (dot(grads, k) + growth * ntdot(g, state)).astype(BF16)
        dk_ref[:, cols] = (tdot(grads, q) + weight * ntdot(v, back)).astype(BF16)
        dv_ref[:, cols] = (tdot(scores, g) + weight * dot(k, back)).astype(BF16)


def run_output(q, k, v, g, rc, states, scores, heads=8):
    n = rc.shape[0]
    tok = pl.BlockSpec((E, heads * E), lambda i: (0, i))
    mat = pl.BlockSpec((2, heads, E, E), lambda i: (0, i, 0, 0))
    return pl.pallas_call(
        functools.partial(output_kernel, heads),
        grid=(n // heads,),
        out_shape=(jax.ShapeDtypeStruct(q.shape, BF16),) * 4,
        in_specs=[tok, tok, tok, tok, pl.BlockSpec((heads, 2, E), lambda i: (i, 0, 0)), mat, mat],
        out_specs=(tok, tok, tok, tok),
        name="chunk_outputs",
    )(q, k, v, g, rc, states, scores)


def on_device(nz, nseq, q, k, v, g, decay):
    states, scores, rc = run_state(q, k, v, g, decay, nz, nseq)
    return run_output(q, k, v, g, rc, states, scores)


def solution(mesh):
    nz = mesh.shape["head"]
    nseq = mesh.shape["seq"]
    tok = P(("seq", "head"), None)
    return jax.shard_map(
        functools.partial(on_device, nz, nseq), mesh=mesh,
        in_specs=(tok, tok, tok, tok, P("head", "seq")),
        out_specs=(tok,) * 4, check_vma=False)
```
